512 devices in a mesh: row: 32 (over z, x), col: 16 (over y, core).
Axes of the slice: x: 4, y: 8, z: 8, core: 2. Of those that a mesh axis runs over, the one named last changes fastest.
Arguments:
- ztrail: float32 [16384, 16384], P('row', 'col'), may hold values from -32 to 32
- panels: float32 [16384, 1024], P('row', 'col'), may hold values from -0.09375 to 0.09375
- window_tiles: float32 [3, 512, 512], P(None, 'row'), may hold values from -3 to 3, as said below
Outputs:
- first_column: float32 [16384, 512], P(('row', 'col'))
- second_column: float32 [16384, 512], P(('row', 'col'))
- corner: float32 [3, 512, 512], P(None, 'row', 'col')
The draws below stay inside these ranges and needn't reach their ends.
Inputs may be any that keep to these rules, and one draw needn't show every extreme that they name: window_tiles[0] and window_tiles[1] are lower triangular with diagonal entries between 1 and 3.
All inputs are finite; a program needn't handle non-finite values.
Results may differ from the reference program's by a relative error of at most 0.00026.
Values sent between devices are 32-bit elements; how exact they have to be, the bound alone decides.
No kernel may reach another device: no remote copies, remote signals or barrier semaphores. Data moves between devices by JAX's collectives and lax.ppermute only.
A program may use at most 64 MiB of HBM per device.

```python
import math
import jax
import jax.numpy as jnp
from jax import lax

TILE = 512
TRAIL = 16384


def draw_ztrail(key, part):
    key_normal, key_diag = jax.random.split(jax.random.fold_in(key, 17), 2)
    gaussian = jnp.clip(jax.random.normal(key_normal, (TRAIL, TRAIL), jnp.float32), -6.0, 6.0)
    coupled = (gaussian + gaussian.T) * (math.sqrt(0.5) / math.sqrt(TRAIL))
    diagonal = jax.random.uniform(key_diag, (TRAIL,), jnp.float32, 0.5, 2.0)
    matrix = coupled + jnp.diag(diagonal)
    return matrix


def draw_window_tiles(key, part):
    key_diag, key_lower, key_couple = jax.random.split(jax.random.fold_in(key, 23), 3)
    width = TILE
    diagonal = jax.random.uniform(key_diag, (2, width), jnp.float32, 1.0, 2.0)
    lower = jnp.clip(jax.random.normal(key_lower, (2, width, width), jnp.float32), -4.0, 4.0) * (0.5 / math.sqrt(width))
    lower = jnp.tril(lower, -1) + diagonal[:, :, None] * jnp.eye(width, dtype=jnp.float32)[None, :, :]
    coupling = jnp.clip(jax.random.normal(key_couple, (1, width, width), jnp.float32), -4.0, 4.0) / math.sqrt(width)
    return jnp.concatenate([lower, coupling], axis=0)


def block_scale(own_key, dims, cuts, least, largest):
    loudness = 1.0
    for position, shards_of in cuts:
        steps = jax.random.uniform(jax.random.fold_in(jax.random.fold_in(own_key, 6), position), (shards_of,), jnp.float32, least / len(cuts), largest / len(cuts))
        loudness = loudness * jnp.repeat(jnp.exp(steps), dims[position] // shards_of).reshape((-1,) + (1,) * (len(dims) - 1 - position))
    return loudness


def scatter_about(rng, dims, scale, most, shards=(), held_as=jnp.bfloat16):
    loudness = block_scale(rng, dims, shards, -0.22, 0.18) if shards else 1.0
    array = jax.random.normal(rng, dims, jnp.float32) * scale * loudness
    return jnp.minimum(jnp.maximum(array, -most), most).astype(held_as)


def setup_inputs(seed: int = 0) -> dict:
    key_of = jax.random.split(jax.random.key(seed), 4)
    ztrail = draw_ztrail(jax.random.fold_in(key_of[3], 71), 0)
    panels = scatter_about(key_of[1], (TRAIL, 2 * TILE), (TRAIL // 4) ** -0.5, 0.09375, ((0, 32), (1, 16)), jnp.float32)
    window_tiles = draw_window_tiles(jax.random.fold_in(key_of[3], 71), 0)
    return {"ztrail": ztrail, "panels": panels, "window_tiles": window_tiles}


def matmul(left_side, right_side):
    return jnp.dot(left_side.astype(jnp.float32), right_side.astype(jnp.float32), precision=lax.Precision.HIGHEST, preferred_element_type=jnp.float32)

def inner_rows(left_rows, right_rows):
    return lax.dot_general(left_rows.astype(jnp.float32), right_rows.astype(jnp.float32), (((0,), (0,)), ((), ())), precision=lax.Precision.HIGHEST, preferred_element_type=jnp.float32)

def right_solve(right_side, lower_tile):
    return lax.linalg.triangular_solve(lower_tile, right_side, left_side=False, lower=True)

def left_solve_t(right_side, lower_tile):
    return lax.linalg.triangular_solve(lower_tile, right_side, left_side=True, lower=True, transpose_a=True)

def corner_tiles(pivot_first, pivot_second, coupling, gram_aa, gram_ab, gram_bb):
    identity = jnp.eye(pivot_first.shape[0], dtype=jnp.float32)
    tile_aa = left_solve_t(right_solve(identity + gram_aa, pivot_first), pivot_first)
    weighed = left_solve_t(gram_ab, pivot_first)
    tile_ab = -right_solve(matmul(tile_aa, coupling) - weighed, pivot_second)
    inner = left_solve_t(identity + gram_bb - inner_rows(coupling, weighed), pivot_second)
    tile_bb = right_solve(inner - inner_rows(tile_ab, coupling), pivot_second)
    return jnp.stack([tile_aa, tile_ab, tile_bb], axis=0)

def reference(ztrail, panels, window_tiles):
    pivot_first = window_tiles[0]
    pivot_second = window_tiles[1]
    coupling = window_tiles[2]
    images = matmul(ztrail, panels)
    first_column = -right_solve(images[:, :TILE], pivot_first)
    second_column = -right_solve(images[:, TILE:] + matmul(first_column, coupling), pivot_second)
    gram_aa = inner_rows(panels[:, :TILE], images[:, :TILE])
    gram_ab = inner_rows(panels[:, :TILE], images[:, TILE:])
    gram_bb = inner_rows(panels[:, TILE:], images[:, TILE:])
    corner = corner_tiles(pivot_first, pivot_second, coupling, gram_aa, gram_ab, gram_bb)
    return (first_column, second_column, corner)
```

```python
import jax
import jax.numpy as jnp
from jax import lax
from jax.experimental import pallas as pl
from jax.experimental.pallas import tpu as pltpu
from jax.sharding import Mesh
from jax.sharding import PartitionSpec as P

ROW = ("z", "x")
COL = ("y", "k")
F32 = jnp.float32
BF16 = jnp.bfloat16
NB = 128


def split(value):
    high = value.astype(BF16)
    return high, (value - high.astype(F32)).astype(BF16)


def dot3(left, right, dims=(((1,), (0,)), ((), ()))):
    def one(a, b):
        return lax.dot_general(a, b, dims, preferred_element_type=F32)
    return one(left[0], right[0]) + (one(left[0], right[1]) + one(left[1], right[0]))


def dot_exact(left, right, dims=(((1,), (0,)), ((), ()))):
    return lax.dot_general(left, right, dims, precision=lax.Precision.HIGHEST, preferred_element_type=F32)


def window_body(core, *refs):
    own, other = refs[:3], refs[3:6]
    panel_own, panel_other, hi_out, lo_out, inv_hi_out, inv_lo_out, panel_hi, panel_lo, tiles = refs[6:]
    k = core[0]
    panel_hi[k], panel_lo[k] = split(panel_own[...])
    panel_hi[1 - k], panel_lo[1 - k] = split(panel_other[...])
    for zz in range(8):
        for xx in range(4):
            base = 64 * zz + 16 * xx
            for m in range(3):
                tiles[m, pl.ds(pl.multiple_of(base + 8 * k, 8), 8), :] = own[m][zz, xx]
                tiles[m, pl.ds(pl.multiple_of(base + 8 * (1 - k), 8), 8), :] = other[m][zz, xx]
    for m in range(3):
        for q in range(4):
            rows = slice(q * NB, (q + 1) * NB)
            high, low = split(tiles[m, rows, :])
            hi_out[m, rows, :] = high
            lo_out[m, rows, :] = low
    row = lax.broadcasted_iota(jnp.int32, (NB, NB), 0)
    col = lax.broadcasted_iota(jnp.int32, (NB, NB), 1)
    eye = row == col
    lowers = [tiles[m, q * NB:(q + 1) * NB, q * NB:(q + 1) * NB] for m in range(2) for q in range(4)]
    inverses = [jnp.where(eye, 1.0 / jnp.where(eye, low, 1.0), 0.0) for low in lowers]
    for s in range(7):
        same = (row >> (s + 1)) == (col >> (s + 1))
        corner = same & (((row >> s) & 1) == 1) & (((col >> s) & 1) == 0)
        parts = [jnp.where(corner, low, 0.0) for low in lowers]
        firsts = [dot_exact(part, inv) for part, inv in zip(parts, inverses)]
        inverses = [inv - dot_exact(inv, first) for first, inv in zip(firsts, inverses)]
    for n, inv in enumerate(inverses):
        high, low = split(inv)
        inv_hi_out[n] = high
        inv_lo_out[n] = low


def prepare_window(core, own, other, panel_own, panel_other):
    return pl.pallas_call(
        window_body,
        out_shape=(
            jax.ShapeDtypeStruct((3, 512, 512), BF16),
            jax.ShapeDtypeStruct((3, 512, 512), BF16),
            jax.ShapeDtypeStruct((8, NB, NB), BF16),
            jax.ShapeDtypeStruct((8, NB, NB), BF16),
            jax.ShapeDtypeStruct((2, 512, 512), BF16),
            jax.ShapeDtypeStruct((2, 512, 512), BF16),
        ),
        in_specs=[pl.BlockSpec(memory_space=pltpu.SMEM)] + [pl.BlockSpec(memory_space=pltpu.VMEM)] * 8,
        scratch_shapes=[pltpu.VMEM((3, 512, 512), F32)],
        name="window",
    )(core, *own, *other, panel_own, panel_other)


def solve_rows(rhs, m, hi, lo, inv_hi, inv_lo):
    solved = [None] * 4
    for p in (3, 2, 1, 0):
        value = rhs[p]
        for q in range(3, p, -1):
            block = (hi[m, q * NB:(q + 1) * NB, p * NB:(p + 1) * NB], lo[m, q * NB:(q + 1) * NB, p * NB:(p + 1) * NB])
            value = value - dot3(solved[q][1], block)
        result = dot3(split(value), (inv_hi[4 * m + p], inv_lo[4 * m + p]))
        solved[p] = (result, split(result))
    return solved


def window_solve(rhs_a, rhs_b, hi, lo, inv_hi, inv_lo):
    solved_a = solve_rows(rhs_a, 0, hi, lo, inv_hi, inv_lo)
    left = [s[1] for s in solved_a]
    left = tuple(jnp.concatenate([part[i] for part in left], axis=1) for i in range(2))
    count = rhs_b[0].shape[0]
    left = tuple(part[:count] for part in left)
    rest = []
    for p in range(4):
        cols = slice(p * NB, (p + 1) * NB)
        rest.append(rhs_b[p] - dot3(left, (hi[2, :, cols], lo[2, :, cols])))
    solved_b = solve_rows(rest, 1, hi, lo, inv_hi, inv_lo)
    return [s[0] for s in solved_a], [s[0] for s in solved_b]


def product_body(core, panel, own, other, out, high, low):
    del core
    t = pl.program_id(0)

    @pl.when(t == 0)
    def _():
        h, l = split(panel[...])
        high[...] = h
        low[...] = l

    @pl.when(t < 2)
    def _():
        out[0] = dot3((high[...], low[...]), split(own[...]))

    @pl.when(t >= 2)
    def _():
        out[0] = dot3((high[...], low[...]), split(other[...]))


def product(core, panel, own, other):
    def place(t, core):
        return (jnp.where(t < 2, 2 * core[0] + t, 2 * (1 - core[0]) + t - 2), 0, 0)
    return pl.pallas_call(
        product_body,
        out_shape=jax.ShapeDtypeStruct((4, 512, 512), F32),
        grid_spec=pltpu.PrefetchScalarGridSpec(
            num_scalar_prefetch=1,
            grid=(4,),
            in_specs=[
                pl.BlockSpec((512, 512), lambda t, core: (0, 0)),
                pl.BlockSpec((512, 512), lambda t, core: (0, jnp.minimum(t, 1))),
                pl.BlockSpec((512, 512), lambda t, core: (0, jnp.maximum(t - 2, 0))),
            ],
            out_specs=pl.BlockSpec((1, 512, 512), place),
            scratch_shapes=[pltpu.VMEM((512, 512), BF16), pltpu.VMEM((512, 512), BF16)],
        ),
        name="product",
    )(core, panel, own, other)


def turn_body(arrived, out):
    total = (arrived[0] + arrived[1]) + (arrived[2] + arrived[3])
    out[...] = total.T


def sum_and_turn(arrived):
    return pl.pallas_call(
        turn_body,
        out_shape=jax.ShapeDtypeStruct((512, 512), F32),
        grid=(4,),
        in_specs=[pl.BlockSpec((4, 512, 128), lambda t: (0, 0, t))],
        out_specs=pl.BlockSpec((128, 512), lambda t: (t, 0)),
        name="turn",
    )(arrived)


def columns_body(first_unit, arrived, hi, lo, inv_hi, inv_lo, columns, to_send):
    halves = []
    for k in range(2):
        total = arrived[k]
        for zz in range(1, 8):
            total = total + arrived[2 * zz + k]
        halves.append(total)
    row = lax.broadcasted_iota(jnp.int32, (8, NB), 0)
    col = lax.broadcasted_iota(jnp.int32, (8, NB), 1)
    unit = first_unit[0] + row
    rhs = []
    for p in range(8):
        lanes = slice(64 * p, 64 * p + 64)
        block = -jnp.concatenate([halves[0][:, lanes], halves[1][:, lanes]], axis=1)
        ones = jnp.where((row < 2) & (col + NB * p == unit), -1.0, 0.0)
        rhs.append(jnp.concatenate([block, ones], axis=0))
    solved_a, solved_b = window_solve(rhs[:4], rhs[4:], hi, lo, inv_hi, inv_lo)
    for p in range(4):
        columns[0, :, p * NB:(p + 1) * NB] = solved_a[p][:32]
        columns[1, :, p * NB:(p + 1) * NB] = solved_b[p][:32]
    for j in range(16):
        p, lanes = j // 4, slice(32 * (j % 4), 32 * (j % 4) + 32)
        a, b = solved_a[p][:, lanes], solved_b[p][:, lanes]
        to_send[j, :16] = jnp.concatenate([a[:16], b[:16], a[16:32], b[16:32]], axis=1)
        to_send[j, 16:] = jnp.concatenate([a[32:40], b[32:40], jnp.zeros((8, 64), F32)], axis=1)


def solve_columns(first_unit, arrived, window):
    return pl.pallas_call(
        columns_body,
        out_shape=(
            jax.ShapeDtypeStruct((2, 32, 512), F32),
            jax.ShapeDtypeStruct((16, 24, 128), F32),
        ),
        in_specs=[pl.BlockSpec(memory_space=pltpu.SMEM)] + [pl.BlockSpec(memory_space=pltpu.VMEM)] * 5,
        name="columns",
    )(first_unit, arrived, *window)


def corner_body(group, arrived, panel_hi, panel_lo, hi, lo, inv_hi, inv_lo, out):
    tops = arrived[:, :16, :64]
    ends = arrived[:, :16, 64:]
    rows = jnp.concatenate([tops, ends], axis=1).reshape(512, 64)
    units = arrived[:, 16:, :64].reshape(128, 64)
    row = lax.broadcasted_iota(jnp.int32, (128, 1024), 0)
    col = lax.broadcasted_iota(jnp.int32, (128, 1024), 1)
    place = 32 * group[0] + 2 * (row >> 3) + (row & 7)
    onehot = jnp.where(((row & 7) < 2) & (col == place), 1.0, 0.0)
    left = split(rows.T)
    across = (((1,), (1,)), ((), ()))
    parts = [dot3(left, (panel_hi[i], panel_lo[i]), across) for i in range(2)]
    pieces = [parts[i][:, 64 * n:64 * n + 64] for n in range(8) for i in range(2)]
    gram = jnp.concatenate(pieces, axis=1)
    one = onehot.astype(BF16)
    high, low = split(units.T)
    def plain(a):
        return jnp.dot(a, one, preferred_element_type=F32)
    gram = -(gram + (plain(high) + plain(low)))
    swapped = jnp.concatenate([gram[32:], gram[:32]], axis=0)
    rhs_a = [swapped[:, p * NB:(p + 1) * NB] for p in range(4)]
    rhs_b = [swapped[:32, 512 + p * NB:512 + (p + 1) * NB] for p in range(4)]
    solved_a, solved_b = window_solve(rhs_a, rhs_b, hi, lo, inv_hi, inv_lo)
    for p in range(4):
        a, b = solved_a[p], solved_b[p]
        block = jnp.concatenate([a[32:], a[:32], b, jnp.zeros((32, NB), F32)], axis=0)
        out[p * NB:(p + 1) * NB, :] = block.T


def solve_corner(group, arrived, panel_hi, panel_lo, window):
    return pl.pallas_call(
        corner_body,
        out_shape=jax.ShapeDtypeStruct((512, 128), F32),
        in_specs=[pl.BlockSpec(memory_space=pltpu.SMEM)] + [pl.BlockSpec(memory_space=pltpu.VMEM)] * 7,
        name="corner",
    )(group, arrived, panel_hi, panel_lo, *window)


def to_all(value, axis):
    count = lax.axis_size(axis)
    return lax.all_to_all(jnp.broadcast_to(value[None], (count, *value.shape)), axis, 0, 0, tiled=True)


def swap_cores(value):
    return lax.ppermute(value, "k", [(0, 1), (1, 0)])


def program(ztrail, panels, window_tiles):
    y, k = lax.axis_index("y"), lax.axis_index("k")
    z, x = lax.axis_index("z"), lax.axis_index("x")
    core = jnp.reshape(k, (1,)).astype(jnp.int32)
    group = jnp.reshape(4 * z + x, (1,)).astype(jnp.int32)
    first_unit = jnp.reshape(32 * (4 * y + x) + 2 * (2 * z + k), (1,)).astype(jnp.int32)

    panel_row = to_all(panels.T, "y").reshape(512, 512)
    other_block = swap_cores(ztrail)

    half = lax.dynamic_slice_in_dim(window_tiles, 8 * k, 8, 1)
    half = lax.all_gather(half, "x", axis=0)
    window_own = []
    for m in range(3):
        window_own.append(lax.all_gather(half[:, m], "z", axis=0))
    window_other = [swap_cores(part) for part in window_own]
    panel_other = swap_cores(panel_row)
    *window, panel_hi, panel_lo = prepare_window(core, window_own, window_other, panel_row, panel_other)

    shares = product(core, panel_row, ztrail, other_block)
    over_x = lax.all_to_all(shares, "x", 0, 0, tiled=True)
    turned = sum_and_turn(over_x).reshape(16, 32, 512)
    over_z = lax.all_to_all(turned, ("z", "k"), 0, 0, tiled=True)
    columns, to_send = solve_columns(first_unit, over_z, window)

    turn = [(8 * i + j, 8 * j + i) for i in range(8) for j in range(8)]
    to_send = lax.ppermute(to_send, ("z", "y"), turn)
    arrived = lax.all_to_all(to_send, COL, 0, 0, tiled=True)
    columns = lax.ppermute(columns, ("z", "y"), turn)
    corner = solve_corner(group, arrived, panel_hi, panel_lo, window)
    shares = lax.all_to_all(corner.reshape(32, 16, 128), ROW, 0, 0, tiled=True)
    block = shares.sum(axis=0)
    corner_block = jnp.stack([block[:, :32], block[:, 32:64], block[:, 64:96]])
    return columns[0], columns[1], corner_block


def solution(mesh):
    torus = Mesh(mesh.devices.reshape(8, 4, 8, 2), ("z", "x", "y", "k"))
    return jax.shard_map(
        program,
        mesh=torus,
        in_specs=(P(ROW, COL), P(ROW, COL), P(None, ROW, None)),
        out_specs=(P((*ROW, *COL), None), P((*ROW, *COL), None), P(None, ROW, COL)),
        check_vma=False,
    )
```

```python
import jax
import jax.numpy as jnp
from jax import lax
from jax.experimental import pallas as pl
from jax.experimental.pallas import tpu as pltpu
from jax.sharding import Mesh
from jax.sharding import PartitionSpec as P

ROW = ("z", "x")
COL = ("y", "k")
F32 = jnp.float32
BF16 = jnp.bfloat16
NB = 128


def split(value):
    high = value.astype(BF16)
    return high, (value - high.astype(F32)).astype(BF16)


def dot3(left, right, dims=(((1,), (0,)), ((), ()))):
    def one(a, b):
        return lax.dot_general(a, b, dims, preferred_element_type=F32)
    return one(left[0], right[0]) + (one(left[0], right[1]) + one(left[1], right[0]))


def dot_exact(left, right, dims=(((1,), (0,)), ((), ()))):
    return lax.dot_general(left, right, dims, precision=lax.Precision.HIGHEST, preferred_element_type=F32)


X_OFFSETS = (0, -1, 1, 2)
RING_OFFSETS = (0, -1, 1, 2, 3, 4, -3, -2)


def window_body(place, own, other, panel_own, panel_other, hi_out, lo_out, inv_hi_out, inv_lo_out, panel_hi, panel_lo, tiles):
    z, x, y, k = place[0], place[1], place[2], place[3]
    for b, off in enumerate(RING_OFFSETS):
        rows = pl.ds(pl.multiple_of(64 * ((y + off) & 7), 64), 64)
        panel_hi[k, rows, :], panel_lo[k, rows, :] = split(panel_own[b])
        panel_hi[1 - k, rows, :], panel_lo[1 - k, rows, :] = split(panel_other[b])
    for b, z_off in enumerate(RING_OFFSETS):
        for a, x_off in enumerate(X_OFFSETS):
            base = 64 * ((z + z_off) & 7) + 16 * ((x + x_off) & 3)
            for m in range(3):
                tiles[m, pl.ds(pl.multiple_of(base + 8 * k, 8), 8), :] = own[b, a, m]
                tiles[m, pl.ds(pl.multiple_of(base + 8 * (1 - k), 8), 8), :] = other[b, a, m]
    row = lax.broadcasted_iota(jnp.int32, (NB, NB), 0)
    col = lax.broadcasted_iota(jnp.int32, (NB, NB), 1)
    eye = row == col
    lowers = [tiles[m, q * NB:(q + 1) * NB, q * NB:(q + 1) * NB] for m in range(2) for q in range(4)]
    inverses = [jnp.where(eye, 1.0 / jnp.where(eye, low, 1.0), 0.0) for low in lowers]
    for s in range(7):
        same = (row >> (s + 1)) == (col >> (s + 1))
        corner = same & (((row >> s) & 1) == 1) & (((col >> s) & 1) == 0)
        parts = [jnp.where(corner, low, 0.0) for low in lowers]
        firsts = [dot_exact(part, inv) for part, inv in zip(parts, inverses)]
        inverses = [inv - dot_exact(inv, first) for first, inv in zip(firsts, inverses)]
    for n, inv in enumerate(inverses):
        high, low = split(inv)
        inv_hi_out[n] = high
        inv_lo_out[n] = low
    for m in range(3):
        for p in range(4):
            first = 0 if m == 2 else (p + 1) * NB
            if first < 512:
                cols = slice(p * NB, (p + 1) * NB)
                block = dot_exact(tiles[m, first:, cols], inverses[4 * min(m, 1) + p])
                hi_out[m, first:, cols], lo_out[m, first:, cols] = split(block)


def prepare_window(place, own, other, panel_own, panel_other):
    return pl.pallas_call(
        window_body,
        out_shape=(
            jax.ShapeDtypeStruct((3, 512, 512), BF16),
            jax.ShapeDtypeStruct((3, 512, 512), BF16),
            jax.ShapeDtypeStruct((8, NB, NB), BF16),
            jax.ShapeDtypeStruct((8, NB, NB), BF16),
            jax.ShapeDtypeStruct((2, 512, 512), BF16),
            jax.ShapeDtypeStruct((2, 512, 512), BF16),
        ),
        in_specs=[pl.BlockSpec(memory_space=pltpu.SMEM)] + [pl.BlockSpec(memory_space=pltpu.VMEM)] * 4,
        scratch_shapes=[pltpu.VMEM((3, 512, 512), F32)],
        name="window",
    )(place, own, other, panel_own, panel_other)


def solve_rows(starts, m, hi, lo):
    values = list(starts)
    solved = [None] * 4
    for p in (3, 2, 1, 0):
        solved[p] = split(values[p])
        rows = slice(p * NB, (p + 1) * NB)
        if p:
            update = dot3(solved[p], (hi[m, rows, :p * NB], lo[m, rows, :p * NB]))
            for n in range(p):
                values[n] = values[n] - update[:, n * NB:(n + 1) * NB]
    return values, solved


def window_solve(rhs_a, rhs_b, hi, lo, inv_hi, inv_lo):
    starts = [dot3(split(b), (inv_hi[p], inv_lo[p])) for p, b in enumerate(rhs_a)]
    starts_b = [dot3(split(b), (inv_hi[4 + p], inv_lo[4 + p])) for p, b in enumerate(rhs_b)]
    values_a, solved_a = solve_rows(starts, 0, hi, lo)
    count = rhs_b[0].shape[0]
    left = tuple(jnp.concatenate([part[i][:count] for part in solved_a], axis=1) for i in range(2))
    update = dot3(left, (hi[2], lo[2]))
    starts_b = [value - update[:, p * NB:(p + 1) * NB] for p, value in enumerate(starts_b)]
    values_b, _ = solve_rows(starts_b, 1, hi, lo)
    return values_a, values_b


def product_body(core, panel, own, other, out, high, low):
    del core
    t = pl.program_id(0)

    @pl.when(t == 0)
    def _():
        h, l = split(panel[...])
        high[...] = h
        low[...] = l

    @pl.when(t < 4)
    def _():
        out[0] = dot3((high[...], low[...]), split(own[...]))

    @pl.when(t >= 4)
    def _():
        out[0] = dot3((high[...], low[...]), split(other[...]))


def product(core, panel, own, other):
    def place(t, core):
        first = jnp.where(t < 4, 2 * core[0], 2 * (1 - core[0]))
        return (first + (t % 4) // 2, 0, t % 2)
    return pl.pallas_call(
        product_body,
        out_shape=jax.ShapeDtypeStruct((4, 512, 512), F32),
        grid_spec=pltpu.PrefetchScalarGridSpec(
            num_scalar_prefetch=1,
            grid=(8,),
            in_specs=[
                pl.BlockSpec((512, 512), lambda t, core: (0, 0)),
                pl.BlockSpec((512, 256), lambda t, core: (0, jnp.minimum(t, 3))),
                pl.BlockSpec((512, 256), lambda t, core: (0, jnp.maximum(t - 4, 0))),
            ],
            out_specs=pl.BlockSpec((1, 512, 256), place),
            scratch_shapes=[pltpu.VMEM((512, 512), BF16), pltpu.VMEM((512, 512), BF16)],
        ),
        name="product",
    )(core, panel, own, other)


def turn_body(arrived, out):
    total = (arrived[0] + arrived[1]) + (arrived[2] + arrived[3])
    out[...] = total.T


def sum_and_turn(arrived):
    return pl.pallas_call(
        turn_body,
        out_shape=jax.ShapeDtypeStruct((512, 512), F32),
        grid=(4,),
        in_specs=[pl.BlockSpec((4, 512, 128), lambda t: (0, 0, t))],
        out_specs=pl.BlockSpec((128, 512), lambda t: (t, 0)),
        name="turn",
    )(arrived)


def columns_body(first_unit, arrived, hi, lo, inv_hi, inv_lo, columns, to_send):
    halves = []
    for k in range(2):
        total = arrived[k]
        for zz in range(1, 8):
            total = total + arrived[2 * zz + k]
        halves.append(total)
    row = lax.broadcasted_iota(jnp.int32, (8, NB), 0)
    col = lax.broadcasted_iota(jnp.int32, (8, NB), 1)
    unit = first_unit[0] + row
    rhs = []
    for p in range(8):
        lanes = slice(64 * p, 64 * p + 64)
        block = -jnp.concatenate([halves[0][:, lanes], halves[1][:, lanes]], axis=1)
        ones = jnp.where((row < 2) & (col + NB * p == unit), -1.0, 0.0)
        rhs.append(jnp.concatenate([block, ones], axis=0))
    solved_a, solved_b = window_solve(rhs[:4], rhs[4:], hi, lo, inv_hi, inv_lo)
    for p in range(4):
        columns[0, :, p * NB:(p + 1) * NB] = solved_a[p][:32]
        columns[1, :, p * NB:(p + 1) * NB] = solved_b[p][:32]
    for j in range(16):
        p, lanes = j // 4, slice(32 * (j % 4), 32 * (j % 4) + 32)
        a, b = solved_a[p][:, lanes], solved_b[p][:, lanes]
        to_send[j, :16] = jnp.concatenate([a[:16], b[:16], a[16:32], b[16:32]], axis=1)
        to_send[j, 16:] = jnp.concatenate([a[32:40], b[32:40], jnp.zeros((8, 64), F32)], axis=1)


def solve_columns(first_unit, arrived, window):
    return pl.pallas_call(
        columns_body,
        out_shape=(
            jax.ShapeDtypeStruct((2, 32, 512), F32),
            jax.ShapeDtypeStruct((16, 24, 128), F32),
        ),
        in_specs=[pl.BlockSpec(memory_space=pltpu.SMEM)] + [pl.BlockSpec(memory_space=pltpu.VMEM)] * 5,
        name="columns",
    )(first_unit, arrived, *window)


def corner_body(group, arrived, panel_hi, panel_lo, hi, lo, inv_hi, inv_lo, out):
    tops = arrived[:, :16, :64]
    ends = arrived[:, :16, 64:]
    rows = jnp.concatenate([tops, ends], axis=1).reshape(512, 64)
    units = arrived[:, 16:, :64].reshape(128, 64)
    row = lax.broadcasted_iota(jnp.int32, (128, 1024), 0)
    col = lax.broadcasted_iota(jnp.int32, (128, 1024), 1)
    place = 32 * group[0] + 2 * (row >> 3) + (row & 7)
    onehot = jnp.where(((row & 7) < 2) & (col == place), 1.0, 0.0)
    left = split(rows.T)
    across = (((1,), (1,)), ((), ()))
    parts = [dot3(left, (panel_hi[i], panel_lo[i]), across) for i in range(2)]
    pieces = [parts[i][:, 64 * n:64 * n + 64] for n in range(8) for i in range(2)]
    gram = jnp.concatenate(pieces, axis=1)
    one = onehot.astype(BF16)
    high, low = split(units.T)
    def plain(a):
        return jnp.dot(a, one, preferred_element_type=F32)
    gram = -(gram + (plain(high) + plain(low)))
    swapped = jnp.concatenate([gram[32:], gram[:32]], axis=0)
    rhs_a = [swapped[:, p * NB:(p + 1) * NB] for p in range(4)]
    rhs_b = [swapped[:32, 512 + p * NB:512 + (p + 1) * NB] for p in range(4)]
    solved_a, solved_b = window_solve(rhs_a, rhs_b, hi, lo, inv_hi, inv_lo)
    for p in range(4):
        a, b = solved_a[p], solved_b[p]
        block = jnp.concatenate([a[32:], a[:32], b, jnp.zeros((32, NB), F32)], axis=0)
        out[p * NB:(p + 1) * NB, :] = block.T


def solve_corner(group, arrived, panel_hi, panel_lo, window):
    return pl.pallas_call(
        corner_body,
        out_shape=jax.ShapeDtypeStruct((512, 128), F32),
        in_specs=[pl.BlockSpec(memory_space=pltpu.SMEM)] + [pl.BlockSpec(memory_space=pltpu.VMEM)] * 7,
        name="corner",
    )(group, arrived, panel_hi, panel_lo, *window)


def to_all(value, axis):
    count = lax.axis_size(axis)
    return lax.all_to_all(jnp.broadcast_to(value[None], (count, *value.shape)), axis, 0, 0, tiled=True)


def swap_cores(value):
    return lax.ppermute(value, "k", [(0, 1), (1, 0)])


def received(value, axis, offset):
    count = lax.axis_size(axis)
    return lax.ppermute(value, axis, [((i + offset) % count, i) for i in range(count)])


def ring_gather(value, axis):
    before, after = received(value, axis, -1), received(value, axis, 1)
    far = received(jnp.stack([before, value, after]), axis, 3)
    near = received(jnp.stack([value, after]), axis, -3)
    return jnp.concatenate([jnp.stack([value, before, after]), far, near])


def program(ztrail, panels, window_tiles):
    y, k = lax.axis_index("y"), lax.axis_index("k")
    z, x = lax.axis_index("z"), lax.axis_index("x")
    core = jnp.reshape(k, (1,)).astype(jnp.int32)
    group = jnp.reshape(4 * z + x, (1,)).astype(jnp.int32)
    place = jnp.stack([z, x, y, k]).astype(jnp.int32)
    first_unit = jnp.reshape(32 * (4 * z + x) + 2 * (2 * y + k), (1,)).astype(jnp.int32)

    flat = panels.T
    panel_row = to_all(flat, "y").reshape(512, 512)
    other_block = swap_cores(ztrail)

    half = lax.dynamic_slice_in_dim(window_tiles, 8 * k, 8, 1)
    half = jnp.stack([half] + [received(half, "x", off) for off in X_OFFSETS[1:]])
    window_own = ring_gather(half, "z")
    window_other = swap_cores(window_own)

    packed = flat.reshape(2, 32, 8, 64).transpose(2, 1, 0, 3).reshape(8, 32, 128)
    packed = lax.all_to_all(packed, "z", 0, 0, tiled=True)
    sub = packed.reshape(8, 32, 2, 64).transpose(2, 1, 0, 3).reshape(64, 512)
    sub_own = ring_gather(sub, "y")
    sub_other = swap_cores(sub_own)
    *window, panel_hi, panel_lo = prepare_window(place, window_own, window_other, sub_own, sub_other)

    shares = product(core, panel_row, ztrail, other_block)
    over_x = lax.all_to_all(shares, "x", 0, 0, tiled=True)
    turned = sum_and_turn(over_x).reshape(16, 32, 512)
    over_z = lax.all_to_all(turned, ("z", "k"), 0, 0, tiled=True)
    columns, to_send = solve_columns(first_unit, over_z, window)

    turn = [(8 * i + j, 8 * j + i) for i in range(8) for j in range(8)]
    arrived = lax.all_to_all(to_send, COL, 0, 0, tiled=True)
    columns = lax.ppermute(columns, ("z", "y"), turn)
    corner = solve_corner(group, arrived, panel_hi, panel_lo, window)
    shares = lax.all_to_all(corner.reshape(32, 16, 128), ROW, 0, 0, tiled=True)
    block = shares.sum(axis=0)
    corner_block = jnp.stack([block[:, :32], block[:, 32:64], block[:, 64:96]])
    return columns[0], columns[1], corner_block


def solution(mesh):
    torus = Mesh(mesh.devices.reshape(8, 4, 8, 2), ("z", "x", "y", "k"))
    return jax.shard_map(
        program,
        mesh=torus,
        in_specs=(P(ROW, COL), P(ROW, COL), P(None, ROW, None)),
        out_specs=(P((*ROW, *COL), None), P((*ROW, *COL), None), P(None, ROW, COL)),
        check_vma=False,
    )
```
